32 devices in a mesh: ctx: 8 (over z, y), head: 4 (over x, core).
Axes of the slice: x: 2, y: 2, z: 4, core: 2. Of those that a mesh axis runs over, the one named last changes fastest.
Arguments:
- query_input: bfloat16 [4096, 4096], P(('ctx', 'head')), may hold values from -6 to 6
- key_input: bfloat16 [4096, 4096], P(('ctx', 'head')), may hold values from -6 to 6
- value_input: bfloat16 [4096, 4096], P(('ctx', 'head')), may hold values from -6 to 6
- cotangent: bfloat16 [4096, 4096], P(('ctx', 'head')), may hold values from -6 to 6
- level_codes: int32 [32, 13, 4096], P('head', None, 'ctx'), may hold values from 0 to 15
Outputs:
- attended: bfloat16 [4096, 4096], P(('ctx', 'head'))
- grad_queries: bfloat16 [4096, 4096], P(('ctx', 'head'))
- grad_keys: bfloat16 [4096, 4096], P(('ctx', 'head'))
- grad_values: bfloat16 [4096, 4096], P(('ctx', 'head'))
The draws below stay inside these ranges and needn't reach their ends.
All inputs are finite; a program needn't handle non-finite values.
Results may differ from the reference program's by a relative error of at most 0.0074.
Values may be sent and summed in bfloat16 or wider, within the bound.
No kernel may reach another device: no remote copies, remote signals or barrier semaphores. Data moves between devices by JAX's collectives and lax.ppermute only.
A program may use at most 128 MiB of HBM per device.

```python
import jax
import jax.numpy as jnp
from jax import lax

H = 32
DH = 128
TOK_DEV = 512
TOKENS = 4096
TOK_BITS = 9
CTX_BITS = 3
NLEV = 13
N_CTX = 8


def set_ends(drawn, own_key, least, largest):
    place = [jax.random.randint(jax.random.fold_in(own_key, axis), (), 0, length) for axis, length in enumerate(drawn.shape)]
    longest = drawn.shape.index(max(drawn.shape))
    next_to = place[:longest] + [(place[longest] + 1) % drawn.shape[longest]] + place[longest + 1:]
    return drawn.at[tuple(place)].set(least).at[tuple(next_to)].set(largest)


def steps_of(key, dims, pieces, low, top_value):
    level, own = 1.0, jax.random.fold_in(key, 6)
    for axis_at, blocks in pieces:
        heights = jnp.exp(jax.random.uniform(jax.random.fold_in(own, axis_at), (blocks,), jnp.float32, low / len(pieces), top_value / len(pieces)))
        level = level * jnp.repeat(heights, dims[axis_at] // blocks).reshape([-1 if axis == axis_at else 1 for axis in range(len(dims))])
    return level


def centred(key, dims, scale, limit, cuts=(), kind=jnp.bfloat16):
    values = scale * jax.random.normal(key, dims, jnp.float32)
    if cuts:
        values = values * steps_of(key, dims, cuts, -0.22, 0.18)
    return jnp.clip(values, -limit, limit).astype(kind)


def setup_inputs(seed: int = 0) -> dict:
    key_list = jax.random.split(jax.random.key(seed), 6)
    return {
        "query_input": centred(key_list[0], (TOKENS, H * DH), 1.0, 6.0, ((0, 32),)),
        "key_input": centred(key_list[1], (TOKENS, H * DH), 1.0, 6.0, ((0, 32),)),
        "value_input": centred(key_list[2], (TOKENS, H * DH), 1.0, 6.0, ((0, 32),)),
        "cotangent": centred(key_list[3], (TOKENS, H * DH), 1.0, 6.0, ((0, 32),)),
        "level_codes": set_ends(jax.random.randint(key_list[4], (H, NLEV, TOKENS), 0, 16), jax.random.fold_in(key_list[4], 1), 0, 15).astype(jnp.int32),
    }


def level_gain(level):
    if level == 0:
        return 1.0
    return 2.0 ** (-(level - 1) / 2.0)


def member_of(owner_block, member_block, bit_index):
    bit_span = 2 ** bit_index
    owner_set = (owner_block // bit_span) % 2 == 1
    member_clear = (member_block // bit_span) % 2 == 0
    same_parent = owner_block // (2 * bit_span) == member_block // (2 * bit_span)
    return jnp.where(owner_set & member_clear & same_parent, 1.0, 0.0).astype(jnp.float32)


def by_block(array):
    return array.reshape(N_CTX, TOK_DEV, H, DH).transpose(0, 2, 1, 3)


def reference(query_input, key_input, value_input, cotangent, level_codes):
    score_scale = DH ** -0.5
    code_blocks = (level_codes.astype(jnp.float32) / 8.0).reshape(H, NLEV, N_CTX, TOK_DEV).transpose(2, 0, 1, 3)
    block_ids = jnp.arange(N_CTX, dtype=jnp.int32)
    query_blocks = by_block(query_input)
    key_blocks = by_block(key_input)
    value_blocks = by_block(value_input)
    cot_blocks = by_block(cotangent)

    def cross_scale(block_index, code_weights):
        return jnp.stack([code_weights[:, TOK_BITS + 1 + bit_index, :] * (score_scale * level_gain(TOK_BITS + 1 + bit_index)) * ((block_index // 2 ** bit_index) % 2).astype(jnp.float32) for bit_index in range(CTX_BITS)])

    def first_pass(inputs):
        block_index, query_heads, key_heads, value_heads, cot_heads, code_weights = inputs
        query_wide = query_heads.astype(jnp.float32)
        state = jnp.einsum("htd,hte->hde", key_heads.astype(jnp.float32), value_heads.astype(jnp.float32))
        row_scale = cross_scale(block_index, code_weights)
        scaled_cot = (row_scale[..., None] * cot_heads.astype(jnp.float32)[None]).astype(jnp.bfloat16)
        grad_state = jnp.einsum("htd,bhte->bhde", query_wide, scaled_cot.astype(jnp.float32))
        return state, grad_state

    states, grad_states = lax.map(first_pass, (block_ids, query_blocks, key_blocks, value_blocks, cot_blocks, code_blocks))
    places = jnp.arange(TOK_DEV, dtype=jnp.int32)
    levels = jnp.zeros((TOK_DEV, TOK_DEV), jnp.int32)
    for bit_index in range(TOK_BITS):
        levels = levels + (places[:, None] // 2 ** bit_index != places[None, :] // 2 ** bit_index).astype(jnp.int32)
    causal = places[None, :] <= places[:, None]

    def second_pass(inputs):
        block_index, query_heads, key_heads, value_heads, cot_heads, code_weights = inputs
        query_wide = query_heads.astype(jnp.float32)
        key_wide = key_heads.astype(jnp.float32)
        value_wide = value_heads.astype(jnp.float32)
        cot_wide = cot_heads.astype(jnp.float32)
        lower_pick = jnp.stack([member_of(block_index, block_ids, bit_index) for bit_index in range(CTX_BITS)])
        bucket = jnp.einsum("be,ehij->bhij", lower_pick, states, precision=lax.Precision.HIGHEST).astype(jnp.bfloat16)
        upper_pick = jnp.stack([member_of(block_ids, block_index, bit_index) for bit_index in range(CTX_BITS)])
        pulled = jnp.einsum("bc,cbhij->hij", upper_pick, grad_states, precision=lax.Precision.HIGHEST).astype(jnp.bfloat16)
        bucket_wide = bucket.astype(jnp.float32)
        pulled_wide = pulled.astype(jnp.float32)
        weight = jnp.zeros((H, TOK_DEV, TOK_DEV), jnp.float32)
        for level_index in range(TOK_BITS + 1):
            weight = jnp.where((levels == level_index)[None], code_weights[:, level_index, :, None] * level_gain(level_index), weight)
        weight = jnp.where(causal[None], weight, 0.0)
        row_scale = cross_scale(block_index, code_weights)
        scores = jnp.einsum("hpd,hsd->hps", query_wide, key_wide)
        attention = (score_scale * weight * scores).astype(jnp.bfloat16).astype(jnp.float32)
        local_out = jnp.einsum("hps,hse->hpe", attention, value_wide)
        cross_out = jnp.sum(row_scale[..., None] * jnp.einsum("hpd,bhde->bhpe", query_wide, bucket_wide), axis=0)
        attended = (local_out + cross_out).astype(jnp.bfloat16)
        dots = jnp.einsum("hpe,hse->hps", cot_wide, value_wide)
        score_grads = (score_scale * weight * dots).astype(jnp.bfloat16).astype(jnp.float32)
        cross_qgrad = jnp.sum(row_scale[..., None] * jnp.einsum("hpe,bhde->bhpd", cot_wide, bucket_wide), axis=0)
        grad_query = (jnp.einsum("hps,hsd->hpd", score_grads, key_wide) + cross_qgrad).astype(jnp.bfloat16)
        grad_key = (jnp.einsum("hps,hpd->hsd", score_grads, query_wide) + jnp.einsum("hse,hde->hsd", value_wide, pulled_wide)).astype(jnp.bfloat16)
        grad_value = (jnp.einsum("hps,hpe->hse", attention, cot_wide) + jnp.einsum("hsd,hde->hse", key_wide, pulled_wide)).astype(jnp.bfloat16)
        return attended, grad_query, grad_key, grad_value

    results = lax.map(second_pass, (block_ids, query_blocks, key_blocks, value_blocks, cot_blocks, code_blocks))

    def unblock(array):
        return array.transpose(0, 2, 1, 3).reshape(TOKENS, H * DH)

    return unblock(results[0]), unblock(results[1]), unblock(results[2]), unblock(results[3])
```

```python
import functools

import jax
import jax.numpy as jnp
from jax import lax
from jax.experimental import pallas as pl
from jax.experimental.pallas import tpu as pltpu
from jax.sharding import PartitionSpec as P


F32 = jnp.float32
BF16 = jnp.bfloat16
CHUNKS = 1
UNROLL = 4


def level_gain(level):
    if level == 0:
        return 1.0
    return 2.0 ** (-(level - 1) / 2.0)


def dot(left, right, left_dim, right_dim):
    return lax.dot_general(
        left, right, (((left_dim,), (right_dim,)), ((), ())), preferred_element_type=F32
    )


def exchanged(block, axis, mask, only=None):
    top = 1 << (mask.bit_length() - 1)
    route = [
        (index, index ^ mask)
        for index in range(lax.axis_size(axis))
        if only is None or bool(index & top) == only
    ]
    return lax.ppermute(block, axis, route)


def plus(left, right):
    return (left.astype(F32) + right.astype(F32)).astype(BF16)


def over_heads(states, side, part, step):
    count = states.shape[0]
    first = (side * CHUNKS + part) * count

    def body(index, carry):
        step(index, first + index)
        return carry

    lax.fori_loop(0, count, body, 0, unroll=min(UNROLL, count))


def lanes_of(head, dim):
    return pl.ds(pl.multiple_of(head * dim, dim), dim)


def sides(info, groups):
    for at, side in enumerate((info[0], 1 - info[0])):
        for part in range(CHUNKS):
            yield side, part, groups[at * CHUNKS + part]


def state_kernel(info, key, value, *outs, dim):
    for side, part, states in sides(info, outs):

        def step(index, head):
            lanes = lanes_of(head, dim)
            states[index] = dot(key[:, lanes], value[:, lanes], 0, 0).astype(BF16)

        over_heads(states, side, part, step)


def grad_state_kernel(info, query, cot, codes, *outs, dim, first, levels, scales):
    count = len(levels)
    for at, (side, part, _) in enumerate(sides(info, outs)):
        states = outs[at * count : (at + 1) * count]

        def step(index, head):
            lanes = lanes_of(head, dim)
            turned = query[:, lanes].T.astype(F32)
            code = codes[head].astype(F32)
            scaled = [
                (turned * (code[first + b : first + b + 1] * (scales[b] * info[1 + b].astype(F32)))).astype(BF16)
                for b in levels
            ]
            grads = dot(jnp.concatenate(scaled, axis=0), cot[:, lanes], 1, 0).astype(BF16)
            for place in range(count):
                states[place][index] = grads[place * dim : (place + 1) * dim]

        over_heads(states[0], side, part, step)


def local_kernel(query, key, value, cot, codes, out, query_grad, key_grad, value_grad, *, dim, scale):
    length = query.shape[0]
    source = lax.broadcasted_iota(jnp.int32, (length, length), 0)
    place = lax.broadcasted_iota(jnp.int32, (length, length), 1)
    apart = jnp.bitwise_xor(source, place)
    top = length.bit_length() - 1
    gains = jnp.full((length, length), scale * level_gain(top) / 8.0, F32)
    for level in range(top - 1, -1, -1):
        gains = jnp.where(apart < 2**level, scale * level_gain(level) / 8.0, gains)
    gains = jnp.where(source <= place, gains, 0.0)

    def body(head, carry):
        lanes = lanes_of(head, dim)
        q, k, v, g = query[:, lanes], key[:, lanes], value[:, lanes], cot[:, lanes]
        code = codes[head].astype(F32)
        weight = jnp.broadcast_to(code[top : top + 1], (length, length))
        for level in range(top - 1, -1, -1):
            weight = jnp.where(apart < 2**level, code[level : level + 1], weight)
        weight = weight * gains
        probs = (weight * dot(k, q, 1, 1)).astype(BF16)
        grads = (weight * dot(v, g, 1, 1)).astype(BF16)
        out[:, lanes] = dot(probs, v, 0, 0)
        query_grad[:, lanes] = dot(grads, k, 0, 0)
        key_grad[:, lanes] = dot(grads, q, 1, 0)
        value_grad[:, lanes] = dot(probs, g, 1, 0)
        return carry

    lax.fori_loop(0, codes.shape[0], body, 0, unroll=2)


def cross_terms(info, codes, head, q, g, out, query_grad, buckets, index, first, levels, scales):
    columns = codes[head].astype(F32).T
    for b, bucket in zip(levels, buckets):
        row_scale = columns[:, first + b : first + b + 1] * (scales[b] * info[1 + b].astype(F32))
        out = out + row_scale * dot(q, bucket[index], 1, 0)
        query_grad = query_grad + row_scale * dot(g, bucket[index], 1, 1)
    return out, query_grad


def cross_kernel(info, query, cot, codes, out_in, query_grad_in, *refs, dim, first, levels, scales):
    count = len(levels)
    out, query_grad = refs[-2:]
    for at, (side, part, _) in enumerate(sides(info, refs)):
        buckets = refs[at * count : (at + 1) * count]

        def step(index, head):
            lanes = lanes_of(head, dim)
            out[:, lanes], query_grad[:, lanes] = cross_terms(
                info, codes, head, query[:, lanes], cot[:, lanes], out_in[:, lanes], query_grad_in[:, lanes],
                buckets, index, first, levels, scales,
            )

        over_heads(buckets[0], side, part, step)


def last_cross_kernel(info, query, cot, codes, out_in, query_grad_in, *refs, dim, first, levels, scales):
    count = len(levels)
    out, query_grad = refs[-2:]
    for at, (side, part, _) in enumerate(sides(info, refs)):
        buckets = refs[at * count : (at + 1) * count]

        @pl.when(pl.program_id(0) == at)
        def _():
            def step(index, head):
                lanes, local = lanes_of(head, dim), lanes_of(index, dim)
                left, right = cross_terms(
                    info, codes, head, query[:, lanes], cot[:, lanes], out_in[:, lanes], query_grad_in[:, lanes],
                    buckets, index, first, levels, scales,
                )
                out[:, local] = left.astype(BF16)
                query_grad[:, local] = right.astype(BF16)

            over_heads(buckets[0], side, part, step)


def pull_kernel(info, key, value, key_grad_in, value_grad_in, *refs, dim):
    key_grad, value_grad = refs[-2:]
    for at, (side, part, _) in enumerate(sides(info, refs)):
        pull, near = refs[2 * at : 2 * at + 2]

        @pl.when(pl.program_id(0) == at)
        def _():
            def step(index, head):
                lanes, local = lanes_of(head, dim), lanes_of(index, dim)
                pulled = plus(pull[index], near[index])
                key_grad[:, local] = (key_grad_in[:, lanes] + dot(value[:, lanes], pulled, 1, 1)).astype(BF16)
                value_grad[:, local] = (value_grad_in[:, lanes] + dot(key[:, lanes], pulled, 1, 0)).astype(BF16)

            over_heads(pull, side, part, step)


def on_device(query, key, value, cot, level_codes):
    length, width = query.shape
    shard_heads, total_levels, _ = level_codes.shape
    head_count, ctx_count = lax.axis_size("head"), lax.axis_size("ctx")
    heads = shard_heads * head_count
    dim = width // heads
    part_heads = heads // (2 * CHUNKS)
    tok_bits = length.bit_length() - 1
    head_bits = head_count.bit_length() - 1
    cross = total_levels - tok_bits - 1
    first = tok_bits + 1
    scale = dim**-0.5
    scales = tuple(scale * level_gain(first + b) / 8.0 for b in range(cross))
    hops = [("head", 2 << bit) for bit in range(head_bits - 1)]
    ctx_bits = ctx_count.bit_length() - 1
    for bit in range(ctx_bits):
        hops.append(("ctx", 3 << (bit - 1) if bit and bit == ctx_bits - 1 else 1 << bit))
    my_head = lax.axis_index("head")
    mine = lax.axis_index("ctx") * head_count + my_head
    bits = [mine // 2**b % 2 for b in range(cross)]
    info = jnp.stack([bits[0], *bits]).astype(jnp.int32)

    padded = -(-total_levels // 16) * 16
    codes = jnp.pad(level_codes.astype(BF16), ((0, 0), (0, padded - total_levels), (0, 0)))
    codes = codes.reshape(shard_heads, padded, head_count, length).transpose(2, 0, 1, 3)
    got = [lax.dynamic_index_in_dim(codes, my_head, keepdims=False)]
    for mask in range(1, head_count):
        got.append(exchanged(lax.dynamic_index_in_dim(codes, my_head ^ mask, keepdims=False), "head", mask))
    groups = []
    for group in range(head_count):
        chosen = got[0]
        for mask in range(1, head_count):
            chosen = jnp.where(my_head ^ group == mask, got[mask], chosen)
        groups.append(chosen)
    codes = jnp.concatenate(groups, axis=0)

    in_smem, in_vmem = pl.BlockSpec(memory_space=pltpu.SMEM), pl.BlockSpec(memory_space=pltpu.VMEM)
    state_out = pltpu.VMEM((part_heads, dim, dim), BF16)
    wide = pltpu.VMEM((length, width), F32)
    narrow = jax.ShapeDtypeStruct((length, width), BF16)

    def run(body, args, outs, work, **grid):
        args = [arg if arg is info else pltpu.with_memory_space_constraint(arg, pltpu.VMEM) for arg in args]
        return pl.pallas_call(
            body,
            in_specs=[in_smem if arg is info else in_vmem for arg in args],
            out_shape=outs,
            cost_estimate=pl.CostEstimate(
                flops=work * heads * length * dim * dim * 2, bytes_accessed=0, transcendentals=0
            ),
            compiler_params=pltpu.CompilerParams(vmem_limit_bytes=12 << 20),
            **(grid or dict(out_specs=[in_vmem] * len(outs))),
        )(*args)

    states = run(functools.partial(state_kernel, dim=dim), [info, key, value], [state_out] * (2 * CHUNKS), 1)
    own, other = states[:CHUNKS], states[CHUNKS:]

    def grad_states(levels):
        count = len(levels)
        flat = run(
            functools.partial(grad_state_kernel, dim=dim, first=first, levels=levels, scales=scales),
            [info, query, cot, codes],
            [state_out] * (2 * CHUNKS * count),
            count,
        )
        for place, b in enumerate(levels):
            grads[b] = [flat[part * count + place] for part in range(2 * CHUNKS)]

    grads = {}
    grad_states((cross - 1,))
    grad_states(tuple(range(cross - 1)))

    parts = range(CHUNKS)
    arrived = [exchanged(other[part], "head", 1) for part in parts]
    buckets = [arrived + [exchanged(own[part], "head", 1, False) for part in parts]]
    running = [plus(own[part], arrived[part]) for part in parts]
    for at, (axis, mask) in enumerate(hops):
        top = at == len(hops) - 1
        arrived = [exchanged(running[part], axis, mask, False if top else None) for part in parts]
        buckets.append(arrived + [exchanged(arrived[part], "head", 1) for part in parts])
        if not top:
            running = [plus(running[part], arrived[part]) for part in parts]

    near = [exchanged(grads[0][CHUNKS + part], "head", 1, True) for part in parts]
    near += [exchanged(grads[0][part], "head", 1, True) for part in parts]
    pulled = [None] * CHUNKS
    for at in range(len(hops) - 1, -1, -1):
        axis, mask = hops[at]
        for part in parts:
            grad = plus(grads[at + 1][part], exchanged(grads[at + 1][CHUNKS + part], "head", 1))
            if pulled[part] is None:
                pulled[part] = exchanged(grad, axis, mask, True)
            else:
                pulled[part] = plus(pulled[part], exchanged(plus(pulled[part], grad), axis, mask))
    pulled += [exchanged(pulled[part], "head", 1) for part in parts]

    out, query_grad, key_grad, value_grad = run(
        functools.partial(local_kernel, dim=dim, scale=scale), [query, key, value, cot, codes], [wide] * 4, 6
    )

    def crossed(body, levels, outs, **grid):
        refs = [buckets[b][part] for part in range(2 * CHUNKS) for b in levels]
        return run(
            functools.partial(body, dim=dim, first=first, levels=levels, scales=scales),
            [info, query, cot, codes, out, query_grad, *refs],
            outs,
            2 * len(levels),
            **grid,
        )

    def block_at(step, core_head):
        side = jnp.where(step < CHUNKS, core_head, 1 - core_head)
        return side * CHUNKS + step % CHUNKS

    def last_grid():
        spec = pl.BlockSpec((length, part_heads * dim), lambda step: (0, block_at(step, lax.axis_index("head") % 2)))
        return dict(grid=(2 * CHUNKS,), out_specs=[spec] * 2)

    split = cross - 1
    out, query_grad = crossed(cross_kernel, tuple(range(split)), [wide] * 2)
    attended, query_grad = crossed(last_cross_kernel, tuple(range(split, cross)), [narrow] * 2, **last_grid())
    refs = [piece for part in range(2 * CHUNKS) for piece in (pulled[part], near[part])]
    key_grad, value_grad = run(
        functools.partial(pull_kernel, dim=dim),
        [info, key, value, key_grad, value_grad, *refs],
        [narrow] * 2,
        2,
        **last_grid(),
    )
    return attended, query_grad, key_grad, value_grad


def solution(mesh):
    rows = P(("ctx", "head"), None)
    return jax.shard_map(
        on_device,
        mesh=mesh,
        in_specs=(rows, rows, rows, rows, P("head", None, "ctx")),
        out_specs=(rows, rows, rows, rows),
        check_vma=False,
    )
```

```python
import functools

import jax
import jax.numpy as jnp
from jax import lax
from jax.experimental import pallas as pl
from jax.experimental.pallas import tpu as pltpu
from jax.sharding import PartitionSpec as P


F32 = jnp.float32
BF16 = jnp.bfloat16
CHUNKS = 2
STATE_BATCH = 16
GRAD_BATCH = 8
LOCAL_BATCH = 8
CROSS_BATCH = 8
LAST_BATCH = 8


def level_gain(level):
    if level == 0:
        return 1.0
    return 2.0 ** (-(level - 1) / 2.0)


def dot(left, right, left_dim, right_dim):
    return lax.dot_general(
        left, right, (((left_dim,), (right_dim,)), ((), ())), preferred_element_type=F32
    )


def exchanged(block, axis, mask, sends=None):
    indices = range(lax.axis_size(axis))
    return lax.ppermute(block, axis, [(index, index ^ mask) for index in indices if sends is None or sends(index)])


def plus(left, right):
    return (left.astype(F32) + right.astype(F32)).astype(BF16)


def lanes_of(head, dim):
    return pl.ds(pl.multiple_of(head * dim, dim), dim)


def first_head(info, group, count):
    side = info[0] if group < CHUNKS else 1 - info[0]
    return (side * CHUNKS + group % CHUNKS) * count


def each(count, step, batch):
    batch = min(batch, count)

    def body(at, carry):
        step([at * batch + place for place in range(batch)])
        return carry

    lax.fori_loop(0, count // batch, body, 0)


def state_kernel(info, key, value, own, other, *, dim):
    half = own.shape[0]
    for states, side in ((own, info[0]), (other, 1 - info[0])):

        def step(ids):
            lanes = [lanes_of(side * half + index, dim) for index in ids]
            pairs = [(key[:, at], value[:, at]) for at in lanes]
            outs = [dot(k, v, 0, 0).astype(BF16) for k, v in pairs]
            for index, out in zip(ids, outs):
                states[index] = out

        each(half, step, STATE_BATCH)


def grad_state_kernel(info, query, cot, codes, *outs, dim, first, levels, scales, half, table):
    for at, side in enumerate((info[0], 1 - info[0])):

        def step(ids):
            heads = [side * half + index for index in ids]
            loads = [(query[:, lanes_of(head, dim)], cot[:, lanes_of(head, dim)], codes[head]) for head in heads]
            results = []
            for q, g, code in loads:
                turned, code = q.T.astype(F32), code.astype(F32)
                scaled = [
                    (turned * (code[first + b : first + b + 1] * (scales[b] * info[1 + b].astype(F32)))).astype(BF16)
                    for b in levels
                ]
                results.append(dot(jnp.concatenate(scaled, axis=0), g, 1, 0).astype(BF16))
            for index, grads in zip(ids, results):
                for place in range(len(levels)):
                    which, offset = table[at][place]
                    outs[which][offset + index] = grads[place * dim : (place + 1) * dim]

        each(half, step, STATE_BATCH if len(levels) == 1 else GRAD_BATCH)


def local_kernel(info, query, key, value, cot, codes, out, query_grad, key_grad, value_grad, *, dim, scale, group):
    length = query.shape[0]
    count = out.shape[1] // dim
    source = lax.broadcasted_iota(jnp.int32, (length, length), 0)
    place = lax.broadcasted_iota(jnp.int32, (length, length), 1)
    apart = jnp.bitwise_xor(source, place)
    top = length.bit_length() - 1
    gains = jnp.full((length, length), scale * level_gain(top) / 8.0, F32)
    for level in range(top - 1, -1, -1):
        gains = jnp.where(apart < 2**level, scale * level_gain(level) / 8.0, gains)
    gains = jnp.where(source <= place, gains, 0.0)
    start = first_head(info, group, count)

    def step(ids):
        loads = []
        for index in ids:
            lanes = lanes_of(start + index, dim)
            loads.append((query[:, lanes], key[:, lanes], value[:, lanes], cot[:, lanes], codes[start + index]))
        scores = [(dot(k, q, 1, 1), dot(v, g, 1, 1)) for q, k, v, g, _ in loads]
        results = []
        for (q, k, v, g, code), (score, grad) in zip(loads, scores):
            code = code.astype(F32)
            weight = jnp.broadcast_to(code[top : top + 1], (length, length))
            for level in range(top - 1, -1, -1):
                weight = jnp.where(apart < 2**level, code[level : level + 1], weight)
            weight = weight * gains
            probs, grads = (weight * score).astype(BF16), (weight * grad).astype(BF16)
            results.append((dot(probs, v, 0, 0), dot(grads, k, 0, 0), dot(grads, q, 1, 0), dot(probs, g, 1, 0)))
        for index, result in zip(ids, results):
            here = lanes_of(index, dim)
            out[:, here], query_grad[:, here], key_grad[:, here], value_grad[:, here] = result

    each(count, step, LOCAL_BATCH)


def cross_step(info, query, cot, codes, out_in, query_grad_in, out, query_grad, buckets, *, dim, start, first, levels, scales):
    def step(ids):
        loads = []
        for index in ids:
            lanes, here = lanes_of(start + index, dim), lanes_of(index, dim)
            states = [bucket[offset + index] for bucket, offset in buckets]
            loads.append(
                (query[:, lanes], cot[:, lanes], out_in[:, here], query_grad_in[:, here], codes[start + index], states)
            )
        results = []
        for q, g, added, grad_added, code, states in loads:
            columns = code.astype(F32).T
            row_scales = [columns[:, first + b : first + b + 1] * (scales[b] * info[1 + b].astype(F32)) for b in levels]
            wide_q = jnp.concatenate([(q.astype(F32) * by).astype(BF16) for by in row_scales], axis=1)
            wide_g = jnp.concatenate([(g.astype(F32) * by).astype(BF16) for by in row_scales], axis=1)
            results.append(
                (
                    added + dot(wide_q, jnp.concatenate(states, axis=0), 1, 0),
                    grad_added + dot(wide_g, jnp.concatenate(states, axis=1), 1, 1),
                )
            )
        for index, (left, right) in zip(ids, results):
            here = lanes_of(index, dim)
            out[:, here] = left.astype(out.dtype)
            query_grad[:, here] = right.astype(query_grad.dtype)

    return step


def cross_kernel(info, query, cot, codes, out_in, query_grad_in, *refs, dim, first, levels, scales, group, table):
    out, query_grad = refs[-2:]
    count = out.shape[1] // dim
    step = cross_step(
        info, query, cot, codes, out_in, query_grad_in, out, query_grad,
        [(refs[which], offset) for which, offset in table],
        dim=dim, start=first_head(info, group, count), first=first, levels=levels, scales=scales,
    )
    each(count, step, CROSS_BATCH)


def last_cross_kernel(info, query, cot, codes, out_in, query_grad_in, bucket, *refs, dim, group, first, levels, scales):
    out, query_grad = refs[-2:]
    count = out_in.shape[1] // dim
    start = first_head(info, group, count)
    step = cross_step(
        info, query, cot, codes, out_in, query_grad_in, out, query_grad, [(bucket, 0)],
        dim=dim, start=start, first=first, levels=levels, scales=scales,
    )
    each(count, step, LAST_BATCH)


def pull_kernel(info, key, value, near, key_grad_in, value_grad_in, pull, *refs, dim, group):
    key_grad, value_grad = refs[-2:]
    count = key_grad_in.shape[1] // dim
    offset = (group + CHUNKS) % (2 * CHUNKS) * count
    start = first_head(info, group, count)

    def step(ids):
        loads = []
        for index in ids:
            lanes, here = lanes_of(start + index, dim), lanes_of(index, dim)
            pulled = plus(pull[index], near[offset + index])
            loads.append((key[:, lanes], value[:, lanes], key_grad_in[:, here], value_grad_in[:, here], pulled))
        results = [
            ((keys + dot(v, pulled, 1, 1)).astype(BF16), (values + dot(k, pulled, 1, 0)).astype(BF16))
            for k, v, keys, values, pulled in loads
        ]
        for index, (left, right) in zip(ids, results):
            here = lanes_of(index, dim)
            key_grad[:, here], value_grad[:, here] = left, right

    each(count, step, LAST_BATCH)


def flush_kernel(info, *refs, body, count, dim, groups):
    *refs, left, right, left_piece, right_piece, done = refs
    fixed = len(refs) - 2 * (len(groups) - 1)
    pieces = [*refs[fixed:], left_piece, right_piece]
    copies = []
    for at, group in enumerate(groups):
        columns = pl.ds(pl.multiple_of(first_head(info, group, count) * dim, count * dim), count * dim)
        for which, out in enumerate((left, right)):
            place = 2 * at + which
            copies.append(pltpu.make_async_copy(pieces[place], out.at[:, columns], done.at[place]))
    for copy in copies[:-2]:
        copy.start()
    body(info, *refs[:fixed], left_piece, right_piece)
    for copy in copies[-2:]:
        copy.start()
    for copy in copies:
        copy.wait()


def on_device(query, key, value, cot, level_codes):
    length, width = query.shape
    shard_heads, total_levels, _ = level_codes.shape
    head_count, ctx_count = lax.axis_size("head"), lax.axis_size("ctx")
    heads = shard_heads * head_count
    dim = width // heads
    half = heads // 2
    count = half // CHUNKS
    groups = range(2 * CHUNKS)
    parts = range(CHUNKS)
    tok_bits = length.bit_length() - 1
    head_bits = head_count.bit_length() - 1
    cross = total_levels - tok_bits - 1
    first = tok_bits + 1
    scale = dim**-0.5
    scales = tuple(scale * level_gain(first + b) / 8.0 for b in range(cross))
    ctx_bits = ctx_count.bit_length() - 1
    hops = [("head", 2 << bit) for bit in range(head_bits - 1)] + [("ctx", 1 << bit) for bit in range(ctx_bits - 1)]
    last, step_bit = 1 << (ctx_bits - 1), 1 << (ctx_bits - 2)
    my_head = lax.axis_index("head")
    mine = lax.axis_index("ctx") * head_count + my_head
    bits = [mine // 2**b % 2 for b in range(cross)]
    info = jnp.stack([bits[0], *bits]).astype(jnp.int32)

    padded = -(-total_levels // 16) * 16
    codes = jnp.pad(level_codes.astype(BF16), ((0, 0), (0, padded - total_levels), (0, 0)))
    codes = codes.reshape(shard_heads, padded, head_count, length).transpose(2, 0, 1, 3)
    got = [lax.dynamic_index_in_dim(codes, my_head, keepdims=False)]
    for mask in range(1, head_count):
        got.append(exchanged(lax.dynamic_index_in_dim(codes, my_head ^ mask, keepdims=False), "head", mask))
    slots = []
    for slot in range(head_count):
        chosen = got[0]
        for mask in range(1, head_count):
            chosen = jnp.where(my_head ^ slot == mask, got[mask], chosen)
        slots.append(chosen)
    codes = jnp.concatenate(slots, axis=0)

    in_smem, in_vmem = pl.BlockSpec(memory_space=pltpu.SMEM), pl.BlockSpec(memory_space=pltpu.VMEM)
    wide = pltpu.VMEM((length, count * dim), F32)

    def state_out(number):
        return pltpu.VMEM((number, dim, dim), BF16)

    def run(body, args, outs, work, **more):
        args = [arg if arg is info else pltpu.with_memory_space_constraint(arg, pltpu.VMEM) for arg in args]
        return pl.pallas_call(
            body,
            in_specs=[in_smem if arg is info else in_vmem for arg in args],
            out_shape=outs,
            cost_estimate=pl.CostEstimate(
                flops=int(work * heads * length * dim * dim * 2), bytes_accessed=0, transcendentals=0
            ),
            compiler_params=pltpu.CompilerParams(vmem_limit_bytes=12 << 20),
            **{"out_specs": [in_vmem] * len(outs), **more},
        )(*args)

    def piece(array, offset):
        return lax.slice_in_dim(array, offset, offset + count)

    def grad_states(levels, table, outs):
        return run(
            functools.partial(
                grad_state_kernel, dim=dim, first=first, levels=levels, scales=scales, half=half, table=table
            ),
            [info, query, cot, codes],
            outs,
            len(levels),
        )

    own, other = run(functools.partial(state_kernel, dim=dim), [info, key, value], [state_out(half)] * 2, 1)
    top_own, top_other = grad_states((cross - 1,), (((0, 0),), ((1, 0),)), [state_out(half), state_out(half)])
    rest = cross - 1
    table = (
        ((1, 0),) + tuple((0, half * at) for at in range(rest - 1)),
        ((1, half),) + tuple((1, half * (2 + at)) for at in range(rest - 1)),
    )
    kept, sent = grad_states(tuple(range(rest)), table, [state_out(half * (rest - 1)), state_out(half * (rest + 1))])

    near_own = exchanged(other, "head", 1)
    near_other = exchanged(own, "head", 1)
    top_partner = exchanged(top_other, "head", 1)
    near_grads = exchanged(sent, "head", 1)

    arrived = {}
    running = {}
    tops = {}
    for part in parts:
        running[part] = plus(piece(own, part * count), piece(near_own, part * count))
    for at, (axis, mask) in enumerate(hops):
        for part in parts:
            sends = (lambda i: not i & step_bit) if at + 1 == len(hops) else None
            arrived[at, part] = exchanged(running[part], axis, mask, sends)
            running[part] = plus(running[part], arrived[at, part])
    for part in parts:
        over = exchanged(running[part], "ctx", last | step_bit, lambda i: not i & last and bool(i & step_bit))
        relay = exchanged(over, "ctx", step_bit, lambda i: i & last and not i & step_bit)
        tops[part] = plus(over, relay)
        tops[part + CHUNKS] = exchanged(tops[part], "head", 1)

    pulled = {}
    for part in parts:
        grad = plus(piece(top_own, part * count), piece(top_partner, part * count))
        relay = exchanged(grad, "ctx", step_bit, lambda i: i & last and i & step_bit)
        grad = plus(grad, relay)
        pulled[part] = exchanged(grad, "ctx", last | step_bit, lambda i: i & last and not i & step_bit)
    offsets = [at * half + part * count for at in range(len(hops)) for part in parts]
    pair_grads = lax.optimization_barrier(
        [plus(piece(kept, offset), piece(near_grads, 2 * half + offset)) for offset in offsets]
    )
    for at in range(len(hops) - 1, -1, -1):
        axis, mask = hops[at]
        for part in parts:
            grad = pair_grads[at * CHUNKS + part]
            grad = plus(pulled[part], grad)
            grad = exchanged(grad, axis, mask, (lambda i: i & step_bit) if at + 1 == len(hops) else None)
            pulled[part] = plus(pulled[part], grad)
    for part in parts:
        pulled[part + CHUNKS] = exchanged(pulled[part], "head", 1)

    sums = {}
    for group in groups:
        sums[group] = list(
            run(
                functools.partial(local_kernel, dim=dim, scale=scale, group=group),
                [info, query, key, value, cot, codes],
                [wide] * 4,
                6 / len(groups),
            )
        )

    for part in parts:
        shared = jnp.concatenate([arrived[at, part] for at in range(len(hops))])
        shared = exchanged(shared, "head", 1)
        for group in (part, part + CHUNKS):
            offset = part * count
            if group == part:
                refs = [near_own] + [arrived[at, part] for at in range(len(hops))]
                table = ((0, offset),) + tuple((1 + at, 0) for at in range(len(hops)))
            else:
                refs = [near_other, shared]
                table = ((0, offset),) + tuple((1, at * count) for at in range(len(hops)))
            sums[group][:2] = run(
                functools.partial(
                    cross_kernel, dim=dim, first=first, levels=tuple(range(rest)), scales=scales, group=group,
                    table=table,
                ),
                [info, query, cot, codes, *sums[group][:2], *refs],
                [wide] * 2,
                2 * rest / len(groups),
            )

    def finished(body, args, **more):
        order = [at for part in parts for at in (part, part + CHUNKS)]
        small = pltpu.VMEM((length, count * dim), BF16)
        pieces = []
        for group in order[:-1]:
            kernel = functools.partial(body, dim=dim, group=group, **more)
            pieces += run(kernel, [info, *args(group)], [small] * 2, 2 / len(groups))
        kernel = functools.partial(body, dim=dim, group=order[-1], **more)
        return run(
            functools.partial(flush_kernel, body=kernel, count=count, dim=dim, groups=order),
            [info, *args(order[-1]), *pieces],
            [jax.ShapeDtypeStruct((length, width), BF16)] * 2,
            2 / len(groups),
            out_specs=[pl.BlockSpec(memory_space=pl.ANY)] * 2,
            scratch_shapes=[small, small, pltpu.SemaphoreType.DMA((2 * len(order),))],
        )

    attended, query_grad = finished(
        last_cross_kernel,
        lambda group: [query, cot, codes, *sums[group][:2], tops[group]],
        first=first,
        levels=(cross - 1,),
        scales=scales,
    )
    key_grad, value_grad = finished(
        pull_kernel, lambda group: [key, value, near_grads, *sums[group][2:], pulled[group]]
    )
    return attended, query_grad, key_grad, value_grad


def solution(mesh):
    rows = P(("ctx", "head"), None)
    return jax.shard_map(
        on_device,
        mesh=mesh,
        in_specs=(rows, rows, rows, rows, P("head", None, "ctx")),
        out_specs=(rows, rows, rows, rows),
        check_vma=False,
    )
```

```python
import functools

import jax
import jax.numpy as jnp
from jax import lax
from jax.experimental import pallas as pl
from jax.experimental.pallas import tpu as pltpu
from jax.sharding import PartitionSpec as P


F32 = jnp.float32
BF16 = jnp.bfloat16
CHUNKS = 2
STATE_BATCH = 16
GRAD_BATCH = 8
LOCAL_BATCH = 8
CROSS_BATCH = 8
LAST_BATCH = 8


def level_gain(level):
    if level == 0:
        return 1.0
    return 2.0 ** (-(level - 1) / 2.0)


def dot(left, right, left_dim, right_dim):
    return lax.dot_general(
        left, right, (((left_dim,), (right_dim,)), ((), ())), preferred_element_type=F32
    )


def exchanged(block, axis, mask, sends=None):
    indices = range(lax.axis_size(axis))
    return lax.ppermute(block, axis, [(index, index ^ mask) for index in indices if sends is None or sends(index)])


def plus(left, right):
    return (left.astype(F32) + right.astype(F32)).astype(BF16)


def lanes_of(head, dim):
    return pl.ds(pl.multiple_of(head * dim, dim), dim)


def first_head(info, group, count):
    side = info[0] if group < CHUNKS else 1 - info[0]
    return (side * CHUNKS + group % CHUNKS) * count


def each(count, step, batch):
    batch = min(batch, count)

    def body(at, carry):
        step([at * batch + place for place in range(batch)])
        return carry

    lax.fori_loop(0, count // batch, body, 0)


def state_kernel(info, key, value, own, other, *, dim):
    half = own.shape[0]
    for states, side in ((own, info[0]), (other, 1 - info[0])):

        def step(ids):
            lanes = [lanes_of(side * half + index, dim) for index in ids]
            pairs = [(key[:, at], value[:, at]) for at in lanes]
            outs = [dot(k, v, 0, 0).astype(BF16) for k, v in pairs]
            for index, out in zip(ids, outs):
                states[index] = out

        each(half, step, STATE_BATCH)


def grad_state_kernel(info, query, cot, codes, *outs, dim, first, levels, scales, half, table):
    for at, side in enumerate((info[0], 1 - info[0])):

        def step(ids):
            heads = [side * half + index for index in ids]
            loads = [(query[:, lanes_of(head, dim)], cot[:, lanes_of(head, dim)], codes[head]) for head in heads]
            results = []
            for q, g, code in loads:
                turned, code = q.T.astype(F32), code.astype(F32)
                scaled = [
                    (turned * (code[first + b : first + b + 1] * (scales[b] * info[1 + b].astype(F32)))).astype(BF16)
                    for b in levels
                ]
                results.append(dot(jnp.concatenate(scaled, axis=0), g, 1, 0).astype(BF16))
            for index, grads in zip(ids, results):
                for place in range(len(levels)):
                    which, offset = table[at][place]
                    outs[which][offset + index] = grads[place * dim : (place + 1) * dim]

        each(half, step, STATE_BATCH if len(levels) == 1 else GRAD_BATCH)


def local_kernel(info, query, key, value, cot, codes, out, query_grad, key_grad, value_grad, *, dim, scale, group):
    length = query.shape[0]
    count = out.shape[1] // dim
    source = lax.broadcasted_iota(jnp.int32, (length, length), 0)
    place = lax.broadcasted_iota(jnp.int32, (length, length), 1)
    apart = jnp.bitwise_xor(source, place)
    top = length.bit_length() - 1
    gains = jnp.full((length, length), scale * level_gain(top) / 8.0, F32)
    for level in range(top - 1, -1, -1):
        gains = jnp.where(apart < 2**level, scale * level_gain(level) / 8.0, gains)
    gains = jnp.where(source <= place, gains, 0.0)
    start = first_head(info, group, count)

    def step(ids):
        loads = []
        for index in ids:
            lanes = lanes_of(start + index, dim)
            loads.append((query[:, lanes], key[:, lanes], value[:, lanes], cot[:, lanes], codes[start + index]))
        scores = [(dot(k, q, 1, 1), dot(v, g, 1, 1)) for q, k, v, g, _ in loads]
        results = []
        for (q, k, v, g, code), (score, grad) in zip(loads, scores):
            code = code.astype(F32)
            weight = jnp.broadcast_to(code[top : top + 1], (length, length))
            for level in range(top - 1, -1, -1):
                weight = jnp.where(apart < 2**level, code[level : level + 1], weight)
            weight = weight * gains
            probs, grads = (weight * score).astype(BF16), (weight * grad).astype(BF16)
            results.append((dot(probs, v, 0, 0), dot(grads, k, 0, 0), dot(grads, q, 1, 0), dot(probs, g, 1, 0)))
        for index, result in zip(ids, results):
            here = lanes_of(index, dim)
            out[:, here], query_grad[:, here], key_grad[:, here], value_grad[:, here] = result

    each(count, step, LOCAL_BATCH)


def cross_step(info, query, cot, codes, out_in, query_grad_in, out, query_grad, buckets, *, dim, start, first, levels, scales):
    def step(ids):
        loads = []
        for index in ids:
            lanes, here = lanes_of(start + index, dim), lanes_of(index, dim)
            states = [bucket[offset + index] for bucket, offset in buckets]
            loads.append((query[:, lanes], cot[:, lanes], out_in[:, here], query_grad_in[:, here], states))
        _, rows, length = codes.shape
        columns = codes[pl.ds(start + ids[0], len(ids))].astype(F32).reshape(len(ids) * rows, length).T
        results = []
        for place, (q, g, added, grad_added, states) in enumerate(loads):
            row_scales = []
            for b in levels:
                column = place * rows + first + b
                row_scales.append(columns[:, column : column + 1] * (scales[b] * info[1 + b].astype(F32)))
            wide_q = jnp.concatenate([(q.astype(F32) * by).astype(BF16) for by in row_scales], axis=1)
            wide_g = jnp.concatenate([(g.astype(F32) * by).astype(BF16) for by in row_scales], axis=1)
            results.append(
                (
                    added + dot(wide_q, jnp.concatenate(states, axis=0), 1, 0),
                    grad_added + dot(wide_g, jnp.concatenate(states, axis=1), 1, 1),
                )
            )
        for index, (left, right) in zip(ids, results):
            here = lanes_of(index, dim)
            out[:, here] = left.astype(out.dtype)
            query_grad[:, here] = right.astype(query_grad.dtype)

    return step


def cross_kernel(info, query, cot, codes, out_in, query_grad_in, *refs, dim, first, levels, scales, group, table):
    out, query_grad = refs[-2:]
    count = out.shape[1] // dim
    step = cross_step(
        info, query, cot, codes, out_in, query_grad_in, out, query_grad,
        [(refs[which], offset) for which, offset in table],
        dim=dim, start=first_head(info, group, count), first=first, levels=levels, scales=scales,
    )
    each(count, step, CROSS_BATCH)


def last_cross_kernel(info, query, cot, codes, out_in, query_grad_in, bucket, *refs, dim, group, first, levels, scales):
    out, query_grad = refs[-2:]
    count = out_in.shape[1] // dim
    start = first_head(info, group, count)
    step = cross_step(
        info, query, cot, codes, out_in, query_grad_in, out, query_grad, [(bucket, 0)],
        dim=dim, start=start, first=first, levels=levels, scales=scales,
    )
    each(count, step, LAST_BATCH)


def pull_kernel(info, key, value, near, key_grad_in, value_grad_in, pull, *refs, dim, group):
    key_grad, value_grad = refs[-2:]
    count = key_grad_in.shape[1] // dim
    offset = (group + CHUNKS) % (2 * CHUNKS) * count
    start = first_head(info, group, count)

    def step(ids):
        loads = []
        for index in ids:
            lanes, here = lanes_of(start + index, dim), lanes_of(index, dim)
            pulled = plus(pull[index], near[offset + index])
            loads.append((key[:, lanes], value[:, lanes], key_grad_in[:, here], value_grad_in[:, here], pulled))
        results = [
            ((keys + dot(v, pulled, 1, 1)).astype(BF16), (values + dot(k, pulled, 1, 0)).astype(BF16))
            for k, v, keys, values, pulled in loads
        ]
        for index, (left, right) in zip(ids, results):
            here = lanes_of(index, dim)
            key_grad[:, here], value_grad[:, here] = left, right

    each(count, step, LAST_BATCH)


def chosen_kernel(info, pull, grad, total, both, *, bit):
    @pl.when(info[1 + bit] == 0)
    def _():
        both[...] = total[...]

    @pl.when(info[1 + bit] != 0)
    def _():
        both[...] = plus(pull[...], grad[...])


def taken_kernel(info, pull, total, swap, pull_out, total_out, *, bit):
    @pl.when(info[1 + bit] == 0)
    def _():
        pull_out[...] = plus(pull[...], swap[...])

    @pl.when(info[1 + bit] != 0)
    def _():
        pull_out[...] = pull[...]

    total_out[...] = plus(total[...], swap[...])


def flush_kernel(info, *refs, body, count, dim, groups):
    *refs, left, right, left_piece, right_piece, done = refs
    fixed = len(refs) - 2 * (len(groups) - 1)
    pieces = [*refs[fixed:], left_piece, right_piece]
    copies = []
    for at, group in enumerate(groups):
        columns = pl.ds(pl.multiple_of(first_head(info, group, count) * dim, count * dim), count * dim)
        for which, out in enumerate((left, right)):
            place = 2 * at + which
            copies.append(pltpu.make_async_copy(pieces[place], out.at[:, columns], done.at[place]))
    for copy in copies[:-2]:
        copy.start()
    body(info, *refs[:fixed], left_piece, right_piece)
    for copy in copies[-2:]:
        copy.start()
    for copy in copies:
        copy.wait()


def on_device(query, key, value, cot, level_codes):
    length, width = query.shape
    shard_heads, total_levels, _ = level_codes.shape
    head_count, ctx_count = lax.axis_size("head"), lax.axis_size("ctx")
    heads = shard_heads * head_count
    dim = width // heads
    half = heads // 2
    count = half // CHUNKS
    groups = range(2 * CHUNKS)
    parts = range(CHUNKS)
    tok_bits = length.bit_length() - 1
    head_bits = head_count.bit_length() - 1
    cross = total_levels - tok_bits - 1
    first = tok_bits + 1
    scale = dim**-0.5
    scales = tuple(scale * level_gain(first + b) / 8.0 for b in range(cross))
    ctx_bits = ctx_count.bit_length() - 1
    hops = [("head", 2 << bit) for bit in range(head_bits - 1)] + [("ctx", 1 << bit) for bit in range(ctx_bits - 1)]
    last, step_bit = 1 << (ctx_bits - 1), 1 << (ctx_bits - 2)
    my_head = lax.axis_index("head")
    mine = lax.axis_index("ctx") * head_count + my_head
    bits = [mine // 2**b % 2 for b in range(cross)]
    info = jnp.stack([bits[0], *bits]).astype(jnp.int32)

    padded = -(-total_levels // 16) * 16
    codes = jnp.pad(level_codes.astype(BF16), ((0, 0), (0, padded - total_levels), (0, 0)))
    codes = codes.reshape(shard_heads, padded, head_count, length).transpose(2, 0, 1, 3)
    got = [lax.dynamic_index_in_dim(codes, my_head, keepdims=False)]
    for mask in range(1, head_count):
        got.append(exchanged(lax.dynamic_index_in_dim(codes, my_head ^ mask, keepdims=False), "head", mask))
    slots = []
    for slot in range(head_count):
        chosen = got[0]
        for mask in range(1, head_count):
            chosen = jnp.where(my_head ^ slot == mask, got[mask], chosen)
        slots.append(chosen)
    codes = jnp.concatenate(slots, axis=0)

    in_smem, in_vmem = pl.BlockSpec(memory_space=pltpu.SMEM), pl.BlockSpec(memory_space=pltpu.VMEM)
    wide = pltpu.VMEM((length, count * dim), F32)

    def state_out(number):
        return pltpu.VMEM((number, dim, dim), BF16)

    def run(body, args, outs, work, **more):
        args = [arg if arg is info else pltpu.with_memory_space_constraint(arg, pltpu.VMEM) for arg in args]
        return pl.pallas_call(
            body,
            in_specs=[in_smem if arg is info else in_vmem for arg in args],
            out_shape=outs,
            cost_estimate=pl.CostEstimate(
                flops=int(work * heads * length * dim * dim * 2), bytes_accessed=0, transcendentals=0
            ),
            compiler_params=pltpu.CompilerParams(vmem_limit_bytes=12 << 20),
            **{"out_specs": [in_vmem] * len(outs), **more},
        )(*args)

    def piece(array, offset):
        return lax.slice_in_dim(array, offset, offset + count)

    def grad_states(levels, table, outs):
        return run(
            functools.partial(
                grad_state_kernel, dim=dim, first=first, levels=levels, scales=scales, half=half, table=table
            ),
            [info, query, cot, codes],
            outs,
            len(levels),
        )

    own, other = run(functools.partial(state_kernel, dim=dim), [info, key, value], [state_out(half)] * 2, 1)
    top_own, top_other = grad_states((cross - 1,), (((0, 0),), ((1, 0),)), [state_out(half), state_out(half)])
    rest = cross - 1
    table = (
        ((1, 0),) + tuple((0, half * at) for at in range(rest - 1)),
        ((1, half),) + tuple((1, half * (2 + at)) for at in range(rest - 1)),
    )
    kept, sent_grads = grad_states(
        tuple(range(rest)), table, [state_out(half * (rest - 1)), state_out(half * (rest + 1))]
    )

    near_own = exchanged(other, "head", 1)
    near_other = exchanged(own, "head", 1)
    top_partner = exchanged(top_other, "head", 1)
    near_grads = exchanged(sent_grads, "head", 1)

    arrived = {}
    running = {}
    tops = {}
    for part in parts:
        running[part] = plus(piece(own, part * count), piece(near_own, part * count))
    for at, (axis, mask) in enumerate(hops[:-1]):
        for part in parts:
            arrived[at, part] = exchanged(running[part], axis, mask)
            running[part] = plus(running[part], arrived[at, part])

    pulled = {}
    for part in parts:
        grad = plus(piece(top_own, part * count), piece(top_partner, part * count))
        relay = exchanged(grad, "ctx", step_bit, lambda i: i & last and i & step_bit)
        grad = plus(grad, relay)
        pulled[part] = exchanged(grad, "ctx", last | step_bit, lambda i: i & last and not i & step_bit)
    offsets = [at * half + part * count for at in range(len(hops)) for part in parts]
    pair_grads = lax.optimization_barrier(
        [plus(piece(kept, offset), piece(near_grads, 2 * half + offset)) for offset in offsets]
    )

    at = len(hops) - 1
    axis, mask = hops[at]
    bit = head_bits + ctx_bits - 2
    for part in parts:
        given = [info, pulled[part], pair_grads[at * CHUNKS + part], running[part]]
        (both,) = run(functools.partial(chosen_kernel, bit=bit), given, [state_out(count)], 0.01)
        arrived[at, part] = exchanged(both, axis, mask)
        given = [info, pulled[part], running[part], arrived[at, part]]
        pulled[part], running[part] = run(functools.partial(taken_kernel, bit=bit), given, [state_out(count)] * 2, 0.01)

    for part in parts:
        over = exchanged(running[part], "ctx", last | step_bit, lambda i: not i & last and bool(i & step_bit))
        relay = exchanged(over, "ctx", step_bit, lambda i: i & last and not i & step_bit)
        tops[part] = plus(over, relay)
        tops[part + CHUNKS] = exchanged(tops[part], "head", 1)

    for at in range(len(hops) - 2, -1, -1):
        axis, mask = hops[at]
        for part in parts:
            grad = plus(pulled[part], pair_grads[at * CHUNKS + part])
            grad = exchanged(grad, axis, mask)
            pulled[part] = plus(pulled[part], grad)
    for part in parts:
        pulled[part + CHUNKS] = exchanged(pulled[part], "head", 1)

    sums = {}
    for group in groups:
        sums[group] = list(
            run(
                functools.partial(local_kernel, dim=dim, scale=scale, group=group),
                [info, query, key, value, cot, codes],
                [wide] * 4,
                6 / len(groups),
            )
        )

    for part in parts:
        shared = jnp.concatenate([arrived[at, part] for at in range(len(hops))])
        shared = exchanged(shared, "head", 1)
        for group in (part, part + CHUNKS):
            offset = part * count
            if group == part:
                refs = [near_own] + [arrived[at, part] for at in range(len(hops))]
                table = ((0, offset),) + tuple((1 + at, 0) for at in range(len(hops)))
            else:
                refs = [near_other, shared]
                table = ((0, offset),) + tuple((1, at * count) for at in range(len(hops)))
            sums[group][:2] = run(
                functools.partial(
                    cross_kernel, dim=dim, first=first, levels=tuple(range(rest)), scales=scales, group=group,
                    table=table,
                ),
                [info, query, cot, codes, *sums[group][:2], *refs],
                [wide] * 2,
                2 * rest / len(groups),
            )

    def finished(body, args, **more):
        order = [at for part in parts for at in (part, part + CHUNKS)]
        small = pltpu.VMEM((length, count * dim), BF16)
        pieces = []
        for group in order[:-1]:
            kernel = functools.partial(body, dim=dim, group=group, **more)
            pieces += run(kernel, [info, *args(group)], [small] * 2, 2 / len(groups))
        kernel = functools.partial(body, dim=dim, group=order[-1], **more)
        return run(
            functools.partial(flush_kernel, body=kernel, count=count, dim=dim, groups=order),
            [info, *args(order[-1]), *pieces],
            [jax.ShapeDtypeStruct((length, width), BF16)] * 2,
            2 / len(groups),
            out_specs=[pl.BlockSpec(memory_space=pl.ANY)] * 2,
            scratch_shapes=[small, small, pltpu.SemaphoreType.DMA((2 * len(order),))],
        )

    attended, query_grad = finished(
        last_cross_kernel,
        lambda group: [query, cot, codes, *sums[group][:2], tops[group]],
        first=first,
        levels=(cross - 1,),
        scales=scales,
    )
    key_grad, value_grad = finished(
        pull_kernel, lambda group: [key, value, near_grads, *sums[group][2:], pulled[group]]
    )
    return attended, query_grad, key_grad, value_grad


def solution(mesh):
    rows = P(("ctx", "head"), None)
    return jax.shard_map(
        on_device,
        mesh=mesh,
        in_specs=(rows, rows, rows, rows, P("head", None, "ctx")),
        out_specs=(rows, rows, rows, rows),
        check_vma=False,
    )
```

```python
import functools

import jax
import jax.numpy as jnp
from jax import lax
from jax.experimental import pallas as pl
from jax.experimental.pallas import tpu as pltpu
from jax.sharding import PartitionSpec as P


F32 = jnp.float32
BF16 = jnp.bfloat16
CHUNKS = 2
STATE_BATCH = 16
GRAD_BATCH = 8
LOCAL_BATCH = 8
CROSS_BATCH = 8
LAST_BATCH = 8


def level_gain(level):
    if level == 0:
        return 1.0
    return 2.0 ** (-(level - 1) / 2.0)


def dot(left, right, left_dim, right_dim):
    return lax.dot_general(
        left, right, (((left_dim,), (right_dim,)), ((), ())), preferred_element_type=F32
    )


def exchanged(block, axis, mask, sends=None):
    indices = range(lax.axis_size(axis))
    return lax.ppermute(block, axis, [(index, index ^ mask) for index in indices if sends is None or sends(index)])


def plus(left, right):
    return (left.astype(F32) + right.astype(F32)).astype(BF16)


def lanes_of(head, dim):
    return pl.ds(pl.multiple_of(head * dim, dim), dim)


def first_head(info, group, count):
    side = info[0] if group < CHUNKS else 1 - info[0]
    return (side * CHUNKS + group % CHUNKS) * count


def each(count, step, batch):
    batch = min(batch, count)

    def body(at, carry):
        step([at * batch + place for place in range(batch)])
        return carry

    lax.fori_loop(0, count // batch, body, 0)


def state_kernel(info, key, value, own, other, keys, values, done, *, dim):
    half = own.shape[0]
    count = half // CHUNKS
    work = []
    for states, side in ((other, 1 - info[0]), (own, info[0])):
        for part in range(CHUNKS):
            at = len(work)
            columns = pl.ds(pl.multiple_of((side * half + part * count) * dim, count * dim), count * dim)
            here = slice(at * count * dim, (at + 1) * count * dim)
            copies = [
                pltpu.make_async_copy(source.at[:, columns], kept.at[:, here], done.at[2 * at + which])
                for which, (source, kept) in enumerate(((key, keys), (value, values)))
            ]
            work.append((states, part * count, at * count, copies))
    for *_, copies in work:
        for copy in copies:
            copy.start()
    for states, offset, place, copies in work:
        for copy in copies:
            copy.wait()

        def step(ids):
            lanes = [lanes_of(place + index, dim) for index in ids]
            pairs = [(keys[:, at], values[:, at]) for at in lanes]
            outs = [dot(k, v, 0, 0).astype(BF16) for k, v in pairs]
            for index, out in zip(ids, outs):
                states[offset + index] = out

        each(count, step, STATE_BATCH)


def grad_state_kernel(info, query, cot, codes, *outs, dim, first, levels, scales, half, table):
    for at, side in enumerate((info[0], 1 - info[0])):

        def step(ids):
            heads = [side * half + index for index in ids]
            loads = [(query[:, lanes_of(head, dim)], cot[:, lanes_of(head, dim)], codes[head]) for head in heads]
            results = []
            for q, g, code in loads:
                turned, code = q.T.astype(F32), code.astype(F32)
                scaled = [
                    (turned * (code[first + b : first + b + 1] * (scales[b] * info[1 + b].astype(F32)))).astype(BF16)
                    for b in levels
                ]
                results.append(dot(jnp.concatenate(scaled, axis=0), g, 1, 0).astype(BF16))
            for index, grads in zip(ids, results):
                for place in range(len(levels)):
                    which, offset = table[at][place]
                    outs[which][offset + index] = grads[place * dim : (place + 1) * dim]

        each(half, step, STATE_BATCH if len(levels) == 1 else GRAD_BATCH)


def local_kernel(info, query, key, value, cot, codes, out, query_grad, key_grad, value_grad, *, dim, scale, group):
    length = query.shape[0]
    count = out.shape[1] // dim
    source = lax.broadcasted_iota(jnp.int32, (length, length), 0)
    place = lax.broadcasted_iota(jnp.int32, (length, length), 1)
    apart = jnp.bitwise_xor(source, place)
    top = length.bit_length() - 1
    gains = jnp.full((length, length), scale * level_gain(top) / 8.0, F32)
    for level in range(top - 1, -1, -1):
        gains = jnp.where(apart < 2**level, scale * level_gain(level) / 8.0, gains)
    gains = jnp.where(source <= place, gains, 0.0)
    start = first_head(info, group, count)

    def step(ids):
        loads = []
        for index in ids:
            lanes = lanes_of(start + index, dim)
            loads.append((query[:, lanes], key[:, lanes], value[:, lanes], cot[:, lanes], codes[start + index]))
        scores = [(dot(k, q, 1, 1), dot(v, g, 1, 1)) for q, k, v, g, _ in loads]
        results = []
        for (q, k, v, g, code), (score, grad) in zip(loads, scores):
            code = code.astype(F32)
            weight = jnp.broadcast_to(code[top : top + 1], (length, length))
            for level in range(top - 1, -1, -1):
                weight = jnp.where(apart < 2**level, code[level : level + 1], weight)
            weight = weight * gains
            probs, grads = (weight * score).astype(BF16), (weight * grad).astype(BF16)
            results.append((dot(probs, v, 0, 0), dot(grads, k, 0, 0), dot(grads, q, 1, 0), dot(probs, g, 1, 0)))
        for index, result in zip(ids, results):
            here = lanes_of(index, dim)
            out[:, here], query_grad[:, here], key_grad[:, here], value_grad[:, here] = result

    each(count, step, LOCAL_BATCH)


def cross_step(info, query, cot, codes, out_in, query_grad_in, out, query_grad, buckets, *, dim, start, first, levels, scales):
    def step(ids):
        loads = []
        for index in ids:
            lanes, here = lanes_of(start + index, dim), lanes_of(index, dim)
            states = [bucket[offset + index] for bucket, offset in buckets]
            loads.append((query[:, lanes], cot[:, lanes], out_in[:, here], query_grad_in[:, here], states))
        _, rows, length = codes.shape
        columns = codes[pl.ds(start + ids[0], len(ids))].astype(F32).reshape(len(ids) * rows, length).T
        results = []
        for place, (q, g, added, grad_added, states) in enumerate(loads):
            row_scales = []
            for b in levels:
                column = place * rows + first + b
                row_scales.append(columns[:, column : column + 1] * (scales[b] * info[1 + b].astype(F32)))
            wide_q = jnp.concatenate([(q.astype(F32) * by).astype(BF16) for by in row_scales], axis=1)
            wide_g = jnp.concatenate([(g.astype(F32) * by).astype(BF16) for by in row_scales], axis=1)
            results.append(
                (
                    added + dot(wide_q, jnp.concatenate(states, axis=0), 1, 0),
                    grad_added + dot(wide_g, jnp.concatenate(states, axis=1), 1, 1),
                )
            )
        for index, (left, right) in zip(ids, results):
            here = lanes_of(index, dim)
            out[:, here] = left.astype(out.dtype)
            query_grad[:, here] = right.astype(query_grad.dtype)

    return step


def cross_kernel(info, query, cot, codes, out_in, query_grad_in, *refs, dim, first, levels, scales, group, table):
    out, query_grad = refs[-2:]
    count = out.shape[1] // dim
    step = cross_step(
        info, query, cot, codes, out_in, query_grad_in, out, query_grad,
        [(refs[which], offset) for which, offset in table],
        dim=dim, start=first_head(info, group, count), first=first, levels=levels, scales=scales,
    )
    each(count, step, CROSS_BATCH)


def last_cross_kernel(info, query, cot, codes, out_in, query_grad_in, bucket, *refs, dim, group, first, levels, scales):
    out, query_grad = refs[-2:]
    count = out_in.shape[1] // dim
    start = first_head(info, group, count)
    step = cross_step(
        info, query, cot, codes, out_in, query_grad_in, out, query_grad, [(bucket, 0)],
        dim=dim, start=start, first=first, levels=levels, scales=scales,
    )
    each(count, step, LAST_BATCH)


def pull_kernel(info, key, value, near, key_grad_in, value_grad_in, pull, *refs, dim, group):
    key_grad, value_grad = refs[-2:]
    count = key_grad_in.shape[1] // dim
    offset = (group + CHUNKS) % (2 * CHUNKS) * count
    start = first_head(info, group, count)

    def step(ids):
        loads = []
        for index in ids:
            lanes, here = lanes_of(start + index, dim), lanes_of(index, dim)
            pulled = plus(pull[index], near[offset + index])
            loads.append((key[:, lanes], value[:, lanes], key_grad_in[:, here], value_grad_in[:, here], pulled))
        results = [
            ((keys + dot(v, pulled, 1, 1)).astype(BF16), (values + dot(k, pulled, 1, 0)).astype(BF16))
            for k, v, keys, values, pulled in loads
        ]
        for index, (left, right) in zip(ids, results):
            here = lanes_of(index, dim)
            key_grad[:, here], value_grad[:, here] = left, right

    each(count, step, LAST_BATCH)


def chosen_kernel(info, pull, grad, total, both, *, bit):
    both[...] = jnp.where(info[1 + bit] != 0, plus(pull[...], grad[...]), total[...])


def taken_kernel(info, pull, total, swap, pull_out, total_out, *, bit):
    came = swap[...]
    pull_out[...] = jnp.where(info[1 + bit] != 0, pull[...], plus(pull[...], came))
    total_out[...] = plus(total[...], came)


def last_kernel(info, *refs, jobs, count, dim, groups):
    *refs, done = refs
    refs = list(refs)

    def take(number):
        taken = refs[:number]
        del refs[:number]
        return taken

    inputs = [take(number) for _, number in jobs]
    pieces = [take(2 * len(groups) - 2) for _ in jobs]
    outs = [take(2) for _ in jobs]
    own = [take(2) for _ in jobs]
    copies = []
    for job in range(len(jobs)):
        for at, group in enumerate(groups):
            columns = pl.ds(pl.multiple_of(first_head(info, group, count) * dim, count * dim), count * dim)
            for which in range(2):
                source = (pieces[job] + own[job])[2 * at + which]
                copies.append(pltpu.make_async_copy(source, outs[job][which].at[:, columns], done.at[len(copies)]))
    each_job = 2 * len(groups)
    for at, copy in enumerate(copies):
        if at % each_job < each_job - 2:
            copy.start()
    for job, (body, _) in enumerate(jobs):
        body(info, *inputs[job], *own[job])
        for copy in copies[(job + 1) * each_job - 2 : (job + 1) * each_job]:
            copy.start()
    for copy in copies:
        copy.wait()


def on_device(query, key, value, cot, level_codes):
    length, width = query.shape
    shard_heads, total_levels, _ = level_codes.shape
    head_count, ctx_count = lax.axis_size("head"), lax.axis_size("ctx")
    heads = shard_heads * head_count
    dim = width // heads
    half = heads // 2
    count = half // CHUNKS
    groups = range(2 * CHUNKS)
    parts = range(CHUNKS)
    tok_bits = length.bit_length() - 1
    head_bits = head_count.bit_length() - 1
    cross = total_levels - tok_bits - 1
    first = tok_bits + 1
    scale = dim**-0.5
    scales = tuple(scale * level_gain(first + b) / 8.0 for b in range(cross))
    ctx_bits = ctx_count.bit_length() - 1
    hops = [("head", 2 << bit) for bit in range(head_bits - 1)] + [("ctx", 1 << bit) for bit in range(ctx_bits - 1)]
    last, step_bit = 1 << (ctx_bits - 1), 1 << (ctx_bits - 2)
    my_head = lax.axis_index("head")
    mine = lax.axis_index("ctx") * head_count + my_head
    bits = [mine // 2**b % 2 for b in range(cross)]
    info = jnp.stack([bits[0], *bits]).astype(jnp.int32)

    padded = -(-total_levels // 16) * 16
    codes = jnp.pad(level_codes.astype(BF16), ((0, 0), (0, padded - total_levels), (0, 0)))
    codes = codes.reshape(shard_heads, padded, head_count, length).transpose(2, 0, 1, 3)
    got = [lax.dynamic_index_in_dim(codes, my_head, keepdims=False)]
    for mask in range(1, head_count):
        got.append(exchanged(lax.dynamic_index_in_dim(codes, my_head ^ mask, keepdims=False), "head", mask))
    slots = []
    for slot in range(head_count):
        chosen = got[0]
        for mask in range(1, head_count):
            chosen = jnp.where(my_head ^ slot == mask, got[mask], chosen)
        slots.append(chosen)
    codes = jnp.concatenate(slots, axis=0)

    in_smem, in_vmem = pl.BlockSpec(memory_space=pltpu.SMEM), pl.BlockSpec(memory_space=pltpu.VMEM)
    wide = pltpu.VMEM((length, count * dim), F32)

    def state_out(number):
        return pltpu.VMEM((number, dim, dim), BF16)

    def run(body, args, outs, work, outside=False, **more):
        space = pltpu.HBM if outside else pltpu.VMEM
        args = [arg if arg is info else pltpu.with_memory_space_constraint(arg, space) for arg in args]
        return pl.pallas_call(
            body,
            out_shape=outs,
            cost_estimate=pl.CostEstimate(
                flops=int(work * heads * length * dim * dim * 2), bytes_accessed=0, transcendentals=0
            ),
            compiler_params=pltpu.CompilerParams(vmem_limit_bytes=12 << 20),
            **{
                "in_specs": [in_smem if arg is info else in_vmem for arg in args],
                "out_specs": [in_vmem] * len(outs),
                **more,
            },
        )(*args)

    def piece(array, offset):
        return lax.slice_in_dim(array, offset, offset + count)

    def grad_states(levels, table, outs):
        return run(
            functools.partial(
                grad_state_kernel, dim=dim, first=first, levels=levels, scales=scales, half=half, table=table
            ),
            [info, query, cot, codes],
            outs,
            len(levels),
        )

    in_hbm = pl.BlockSpec(memory_space=pltpu.HBM)
    fetched = pltpu.VMEM((length, width), BF16)
    own, other = run(
        functools.partial(state_kernel, dim=dim),
        [info, key, value],
        [state_out(half)] * 2,
        1,
        outside=True,
        in_specs=[in_smem, in_hbm, in_hbm],
        scratch_shapes=[fetched, fetched, pltpu.SemaphoreType.DMA((4 * CHUNKS,))],
    )
    top_own, top_other = grad_states((cross - 1,), (((0, 0),), ((1, 0),)), [state_out(half), state_out(half)])
    rest = cross - 1
    table = (
        ((1, 0),) + tuple((0, half * at) for at in range(rest - 1)),
        ((1, half),) + tuple((1, half * (2 + at)) for at in range(rest - 1)),
    )
    kept, sent_grads = grad_states(
        tuple(range(rest)), table, [state_out(half * (rest - 1)), state_out(half * (rest + 1))]
    )

    near_own = exchanged(other, "head", 1)
    near_other = exchanged(own, "head", 1)
    top_partner = exchanged(top_other, "head", 1)
    near_grads = exchanged(sent_grads, "head", 1)

    arrived = {}
    running = {}
    tops = {}
    for part in parts:
        running[part] = plus(piece(own, part * count), piece(near_own, part * count))
    for at, (axis, mask) in enumerate(hops[:-1]):
        for part in parts:
            arrived[at, part] = exchanged(running[part], axis, mask)
            running[part] = plus(running[part], arrived[at, part])

    pulled = {}
    for part in parts:
        grad = plus(piece(top_own, part * count), piece(top_partner, part * count))
        relay = exchanged(grad, "ctx", step_bit, lambda i: i & last and i & step_bit)
        grad = plus(grad, relay)
        pulled[part] = exchanged(grad, "ctx", last | step_bit, lambda i: i & last and not i & step_bit)
    offsets = [at * half + part * count for at in range(len(hops)) for part in parts]
    pair_grads = lax.optimization_barrier(
        [plus(piece(kept, offset), piece(near_grads, 2 * half + offset)) for offset in offsets]
    )

    at = len(hops) - 1
    axis, mask = hops[at]
    bit = head_bits + ctx_bits - 2
    for part in parts:
        given = [info, pulled[part], pair_grads[at * CHUNKS + part], running[part]]
        (both,) = run(functools.partial(chosen_kernel, bit=bit), given, [state_out(count)], 0.01)
        arrived[at, part] = exchanged(both, axis, mask)
        given = [info, pulled[part], running[part], arrived[at, part]]
        pulled[part], running[part] = run(functools.partial(taken_kernel, bit=bit), given, [state_out(count)] * 2, 0.01)

    for part in parts:
        over = exchanged(running[part], "ctx", last | step_bit, lambda i: not i & last and bool(i & step_bit))
        relay = exchanged(over, "ctx", step_bit, lambda i: i & last and not i & step_bit)
        tops[part] = plus(over, relay)
        tops[part + CHUNKS] = exchanged(tops[part], "head", 1)

    for at in range(len(hops) - 2, -1, -1):
        axis, mask = hops[at]
        for part in parts:
            grad = plus(pulled[part], pair_grads[at * CHUNKS + part])
            grad = exchanged(grad, axis, mask)
            pulled[part] = plus(pulled[part], grad)
    for part in parts:
        pulled[part + CHUNKS] = exchanged(pulled[part], "head", 1)

    sums = {}
    for group in groups:
        sums[group] = list(
            run(
                functools.partial(local_kernel, dim=dim, scale=scale, group=group),
                [info, query, key, value, cot, codes],
                [wide] * 4,
                6 / len(groups),
            )
        )

    for part in parts:
        shared = jnp.concatenate([arrived[at, part] for at in range(len(hops))])
        shared = exchanged(shared, "head", 1)
        for group in (part, part + CHUNKS):
            offset = part * count
            if group == part:
                refs = [near_own] + [arrived[at, part] for at in range(len(hops))]
                table = ((0, offset),) + tuple((1 + at, 0) for at in range(len(hops)))
            else:
                refs = [near_other, shared]
                table = ((0, offset),) + tuple((1, at * count) for at in range(len(hops)))
            sums[group][:2] = run(
                functools.partial(
                    cross_kernel, dim=dim, first=first, levels=tuple(range(rest)), scales=scales, group=group,
                    table=table,
                ),
                [info, query, cot, codes, *sums[group][:2], *refs],
                [wide] * 2,
                2 * rest / len(groups),
            )

    group_order = [at for part in parts for at in (part, part + CHUNKS)]
    small = pltpu.VMEM((length, count * dim), BF16)
    jobs = (
        (
            functools.partial(last_cross_kernel, dim=dim, first=first, levels=(cross - 1,), scales=scales),
            lambda group: [query, cot, codes, *sums[group][:2], tops[group]],
        ),
        (
            functools.partial(pull_kernel, dim=dim),
            lambda group: [key, value, near_grads, *sums[group][2:], pulled[group]],
        ),
    )
    inputs, pieces, bodies = [], [], []
    for body, args in jobs:
        for group in group_order[:-1]:
            kernel = functools.partial(body, group=group)
            pieces += run(kernel, [info, *args(group)], [small] * 2, 2 / len(groups))
        bodies.append((functools.partial(body, group=group_order[-1]), len(args(group_order[-1]))))
        inputs += args(group_order[-1])
    attended, query_grad, key_grad, value_grad = run(
        functools.partial(last_kernel, jobs=bodies, count=count, dim=dim, groups=group_order),
        [info, *inputs, *pieces],
        [jax.ShapeDtypeStruct((length, width), BF16)] * 4,
        4 / len(groups),
        out_specs=[in_hbm] * 4,
        scratch_shapes=[small] * 4 + [pltpu.SemaphoreType.DMA((4 * len(group_order),))],
    )
    return attended, query_grad, key_grad, value_grad


def solution(mesh):
    rows = P(("ctx", "head"), None)
    return jax.shard_map(
        on_device,
        mesh=mesh,
        in_specs=(rows, rows, rows, rows, P("head", None, "ctx")),
        out_specs=(rows, rows, rows, rows),
        check_vma=False,
    )
```
